256 devices in a mesh: row: 32 (over y, z), col: 8 (over x, core).
Axes of the slice: x: 4, y: 4, z: 8, core: 2. Of those that a mesh axis runs over, the one named last changes fastest.
Arguments:
- features: bfloat16 [49152, 4096], P(('row', 'col')), may hold values from -24 to 24
- cotangent: bfloat16 [49152, 8192], P(('row', 'col')), may hold values from -0.02734375 to 0.02734375
Outputs:
- weight_grad: float32 [4096, 8192], P('row', 'col')
The draws below stay inside these ranges and needn't reach their ends.
All inputs are finite; a program needn't handle non-finite values.
Results may differ from the reference program's by a relative error of at most 0.0003.
Values may be sent and summed in bfloat16 or wider, within the bound.
A program may use at most 256 MiB of HBM per device.

```python
import jax
import jax.numpy as jnp
from jax import lax

DIN = 4096
DOUT = 8192
TOK_DEV = 192
TOKENS = 49152
N_ROW = 32
N_COL = 8


def strengthened(array, rng, source, target, blocks, factor):
    owner, partner = [(jnp.arange(array.shape[position]) // (array.shape[position] // blocks)).reshape([-1 if axis == position else 1 for axis in range(array.ndim)]) for position in (source, target)]
    chosen = jax.random.permutation(rng, blocks)[partner]
    strong = (owner == chosen) | (owner == (partner + blocks // 2) % blocks)
    return jnp.where(strong, factor * array, array)


def block_levels(own_key, extent, split, low, high):
    def one(position, shards_of):
        heights = jax.random.uniform(jax.random.fold_in(jax.random.fold_in(own_key, 6), position), (shards_of,), jnp.float32, low / len(split), high / len(split))
        return jnp.repeat(jnp.exp(heights), extent[position] // shards_of).reshape((-1,) + (1,) * (len(extent) - position - 1))

    level = one(*split[0])
    for cut in split[1:]:
        level = level * one(*cut)
    return level


def centred(stream_key, shape, width, most, cuts=(), dtype=jnp.bfloat16):
    values = jax.random.normal(stream_key, shape, jnp.float32) * width
    if len(cuts) > 0:
        values = block_levels(stream_key, shape, cuts, -0.22, 0.18) * values
    return jnp.clip(values, min=-most, max=most).astype(dtype)


def heavy_noise(key, shape, deviation, bound, shards, heavy, kind=jnp.bfloat16):
    drawn = deviation * jax.random.normal(key, shape, jnp.float32)
    if shards:
        drawn = drawn * block_levels(key, shape, shards, -0.22, 0.18)
    return jnp.clip(strengthened(drawn, jax.random.fold_in(key, 3), *heavy), -bound, bound).astype(kind)


def setup_inputs(seed: int = 0) -> dict:
    key_of = jax.random.split(jax.random.key(seed), 3)
    features = heavy_noise(key_of[0], (TOKENS, DIN), 1.0, 24.0, ((0, 256),), (0, 1, 256, 6.0))
    cotangent = centred(key_of[1], (TOKENS, DOUT), TOKENS ** -0.5, 0.02734375, ((0, 256),))
    return {"features": features, "cotangent": cotangent}


def reference(features, cotangent):
    block_rows = TOK_DEV * N_COL
    feature_blocks = features.reshape(N_ROW, block_rows, DIN)
    cotangent_blocks = cotangent.reshape(N_ROW, block_rows, DOUT)

    def accumulate(running, paired):
        left = paired[0].astype(jnp.float32)
        right = paired[1].astype(jnp.float32)
        return running + jnp.dot(left.T, right, precision=lax.Precision.HIGHEST), None

    initial = jnp.zeros((DIN, DOUT), jnp.float32)
    weight_grad, unused = lax.scan(accumulate, initial, (feature_blocks, cotangent_blocks))
    return weight_grad
```

```python
import jax
import jax.numpy as jnp
from jax import lax
from jax.experimental import pallas as pl
from jax.experimental.pallas import tpu as pltpu
from jax.sharding import PartitionSpec as P

NX, NY, NZ = 4, 4, 8
TOK = 192
HALF = TOK // 2
GROUP = 8 * TOK
COLS = 1024
BLK = 128
CHUNK = NY * BLK
N = NZ
TILE = 128
H = COLS // 2

POWER = 32
LOW = 2.0**-3.9
SPAN = 2.0**3.9 - 2.0**-3.9
PAD = 16

f32, bf16 = jnp.float32, jnp.bfloat16


def rows(start, size):
    return pl.ds(pl.multiple_of(start, 32), size)


def tile(t):
    return pl.ds(pl.multiple_of(t * TILE, TILE), TILE)


def encode(read, first, tiles, message):
    def widest(t, most):
        value = jnp.abs(read(first + t))
        return jnp.maximum(most, jnp.max(value.reshape(TILE // 8, 8, BLK), axis=0))

    most = lax.fori_loop(0, tiles, widest, jnp.zeros((8, BLK), f32))
    most = jnp.maximum(jnp.max(most, axis=0, keepdims=True) * 1.01, 1e-30)
    most = jnp.broadcast_to(most, (PAD, BLK)).astype(bf16)
    message[pl.ds(tiles * TILE, PAD), :] = most
    scale = SPAN / most.astype(f32)[:1]

    def code(t, _):
        value = read(first + t)
        power = jnp.abs(value) * scale + LOW
        for _ in range(5):
            power = power * power
        message[tile(t), :] = jnp.where(value < 0, -power, power).astype(bf16)
        return 0

    lax.fori_loop(0, tiles, code, 0)


def decoder(message, tiles):
    scale = message[pl.ds(tiles * TILE, PAD), :].astype(f32)[:1] * (1.0 / SPAN)

    def decode(t):
        value = message[tile(t), :].astype(f32)
        root = jnp.exp2(jnp.log(jnp.abs(value)) * (1.4426950408889634 / POWER))
        size = (root - LOW) * scale
        return jnp.where(value < 0, -size, size)

    return decode


def kernel(
    f_in, c_in, out, f_all, c_all, relay, ct, pt, s1, r1, s2, r2, zs, zr,
    f_own, c_own, c_out, c_far_out, c_get, c_far, c_relay,
    f_out, f_pass, f_relay, f_get, y1_out, y1_get, y2_out, y2_get, z_out, z_get,
):
    row, col = lax.axis_index("row"), lax.axis_index("col")
    y, z = lax.div(row, NZ), lax.rem(row, NZ)
    x, k = lax.div(col, 2), lax.rem(col, 2)

    def on_x(step, core):
        return {"row": row, "col": lax.rem(x + step + NX, NX) * 2 + core}

    def on_y(step):
        return {"row": lax.rem(y + step + NY, NY) * NZ + z, "col": col}

    def on_z(step):
        return {"row": y * NZ + lax.rem(z + step + NZ, NZ), "col": col}

    def place(step, core):
        return lax.rem(x + step + NX, NX) * 2 + core

    def send(src, dst, out_sem, get_sem, to):
        return pltpu.make_async_remote_copy(
            src_ref=src, dst_ref=dst, send_sem=out_sem, recv_sem=get_sem,
            device_id=to, device_id_type=pl.DeviceIdType.MESH,
        )

    partner = on_x(0, 1 - k)

    def offset(n):
        far = N // 2 - lax.div(n + 1, 2)
        return lax.rem(z + far * (2 * lax.rem(n, 2) - 1) + NZ, NZ)

    def own_features(n, _):
        for yy in range(NY):
            at = pl.multiple_of((yy * NZ + offset(n)) * BLK, BLK)
            pltpu.make_async_copy(
                f_in.at[:, pl.ds(at, BLK)],
                f_all.at[n, rows(col * TOK, TOK), pl.ds(yy * BLK, BLK)],
                f_own.at[n],
            ).start()
        return 0

    def columns(device):
        return pl.ds(pl.multiple_of(device * COLS, COLS), COLS)

    lax.fori_loop(0, N, own_features, 0)
    keep = pltpu.make_async_copy(
        c_in.at[:, columns(col)], c_all.at[rows(col * TOK, TOK), :], c_own.at[0]
    )
    keep.start()

    barrier = pltpu.get_barrier_semaphore()
    peers = [partner] + [on_x(d, c) for d in (1, -1) for c in (0, 1)]
    peers += [on_y(1), on_y(-1), on_z(1), on_z(-1)]
    for peer in peers:
        pl.semaphore_signal(
            barrier, inc=1, device_id=peer, device_id_type=pl.DeviceIdType.MESH
        )
    pl.semaphore_wait(barrier, len(peers))

    ways = ((0, 1), (1, -1))

    def far_first(way, d, c):
        return send(
            c_in.at[pl.ds(way * HALF, HALF), columns(place(2, c))],
            relay.at[way * 2 + c], c_far_out.at[way * 2 + c], c_relay.at[way * 2 + c],
            on_x(d, k),
        )

    def far_second(way, d, c):
        at = rows(place(-d, k) * TOK + way * HALF, HALF)
        return send(
            relay.at[way * 2 + c], c_all.at[at, :],
            c_far_out.at[4 + way * 2 + c], c_far.at[way * 2 + k], on_x(d, c),
        )

    def near(step, c, slot):
        return send(
            c_in.at[:, columns(place(step, c))], c_all.at[rows(col * TOK, TOK), :],
            c_out.at[slot], c_get.at[col], on_x(step, c),
        )

    nears = [near(d, c, way * 2 + c) for way, d in ways for c in (0, 1)]
    nears.append(near(0, 1 - k, 4))
    for way, d in ways:
        for c in (0, 1):
            far_first(way, d, c).start()
    for copy in nears:
        copy.start()

    def block(n, device):
        return f_all.at[n, rows(device * TOK, TOK), :]

    def pass_on(n, device, out_sem, to):
        return send(block(n, device), block(n, device), out_sem, f_get.at[n, device], to)

    def own_out(n):
        return [
            pass_on(n, col, f_out.at[n, 0], on_x(1, k)),
            pass_on(n, col, f_out.at[n, 1], on_x(-1, k)),
            pass_on(n, col, f_out.at[n, 2], partner),
        ]

    def to_partner(n, step, slot):
        return pass_on(n, place(step, k), f_pass.at[n, slot], partner)

    def relayed(n):
        d = 1 - 2 * lax.rem(n, 2)
        return pass_on(n, place(-d, k), f_relay.at[n], on_x(d, k))

    def arrived(n, device):
        pass_on(n, device, f_out.at[n, 0], f_partner).wait_recv()

    f_partner = partner

    def x0(n):
        pltpu.make_async_copy(
            f_in.at[:, pl.ds(0, CHUNK)], block(n, col), f_own.at[n]
        ).wait()
        for copy in own_out(n):
            copy.start()

    def x1(n):
        arrived(n, place(1, k))
        arrived(n, place(-1, k))
        relayed(n).start()
        to_partner(n, 1, 0).start()
        to_partner(n, -1, 1).start()

    def x2(n):
        arrived(n, place(2, k))
        to_partner(n, 2, 2).start()

    x0(0)
    for way, d in ways:
        for c in (0, 1):
            far_first(way, d, c).wait_recv()
            far_second(way, d, c).start()
    x0(1)
    x0(2)
    x1(0)
    x2(0)

    keep.wait()
    for step, c in ((0, 1 - k), (1, 0), (1, 1), (-1, 0), (-1, 1)):
        send(
            c_in.at[:, columns(0)], c_all.at[rows(0, TOK), :],
            c_out.at[0], c_get.at[place(step, c)], partner,
        ).wait_recv()
    for i in range(4):
        send(
            relay.at[i], c_all.at[rows(0, HALF), :], c_out.at[0], c_far.at[i], partner
        ).wait_recv()

    def transpose(t, _):
        ct[:, tile(t)] = c_all[tile(t), :].T
        return 0

    lax.fori_loop(0, GROUP // TILE, transpose, 0)

    y_up, y_down = lax.rem(y + 1, NY), lax.rem(y + 3, NY)
    y_far = lax.rem(y + 2, NY)

    def first_out(n):
        return [
            send(s1.at[n, i], r1.at[n, i], y1_out.at[n, i], y1_get.at[n, i], on_y(d))
            for i, d in ways
        ]

    def second_out(n):
        return [
            send(s2.at[n, i], r2.at[n, i], y2_out.at[n, i], y2_get.at[n, i], on_y(d))
            for i, d in ways
        ]

    def a(n):
        slot = lax.rem(n, 4)
        for c in range(NX):
            arrived(n, c * 2 + 1 - k)

        def product(m, _):
            at = pl.ds(pl.multiple_of(m * 256, 256), 256)
            value = jnp.dot(ct[at, :], f_all[n], preferred_element_type=f32)
            for yy in range(NY):
                pt[slot, yy, at, :] = value[:, yy * BLK : (yy + 1) * BLK]
            return 0

        lax.fori_loop(0, COLS // 256, product, 0)
        half = H // TILE
        for i in (0, 1):
            encode(lambda t: pt[slot, y_far, tile(t), :], i * half, half, s1.at[n, i])
        for copy in first_out(n):
            copy.start()

    def b(n):
        slot = lax.rem(n, 4)
        half = H // TILE
        arriving = first_out(n)
        leaving = second_out(n)
        for i, target in ((0, y_up), (1, y_down)):
            arriving[i].wait_recv()
            decode = decoder(r1.at[n, i], half)

            def add(t, _):
                at = tile(i * half + t)
                pt[slot, target, at, :] += decode(t)
                return 0

            lax.fori_loop(0, half, add, 0)
            encode(lambda t: pt[slot, target, tile(t), :], 0, COLS // TILE, s2.at[n, i])
            leaving[i].start()

    whole = COLS + PAD
    part = H + PAD

    def z_half(i, d):
        return send(
            zs.at[i * 7, pl.ds(0, part), :], zr.at[i * 7, pl.ds(0, part), :],
            z_out.at[i * 7], z_get.at[i * 7], on_z(d),
        )

    def z_whole(n):
        d = 2 * lax.rem(n, 2) - 1
        return send(zs.at[n], zr.at[n], z_out.at[n], z_get.at[n], on_z(d))

    def c(n):
        slot = lax.rem(n, 4)
        half = H // TILE
        arriving = second_out(n)
        arriving[0].wait_recv()
        arriving[1].wait_recv()
        up = decoder(r2.at[n, 0], COLS // TILE)
        down = decoder(r2.at[n, 1], COLS // TILE)

        def total(t, _):
            pt[slot, y, tile(t), :] += up(t) + down(t)
            return 0

        lax.fori_loop(0, COLS // TILE, total, 0)

        def read(t):
            return pt[slot, y, tile(t), :]

        def join(message, tiles, first):
            decode = decoder(message, tiles)

            def add(t, _):
                pt[slot, y, tile(first + t), :] += decode(t)
                return 0

            lax.fori_loop(0, tiles, add, 0)

        @pl.when(n == 0)
        def _():
            for i, d in ways:
                encode(read, i * half, half, zs.at[i * 7])
                z_half(i, d).start()

        @pl.when(n == 1)
        def _():
            z_half(0, 1).wait_recv()
            join(zr.at[0], half, 0)

        @pl.when(n == 2)
        def _():
            z_half(1, -1).wait_recv()
            join(zr.at[7], half, half)

        @pl.when(n >= 3)
        def _():
            z_whole(n - 2).wait_recv()
            join(zr.at[n - 2], COLS // TILE, 0)

        @pl.when((n >= 1) & (n < N - 1))
        def _():
            encode(read, 0, COLS // TILE, zs.at[n])
            z_whole(n).start()

        @pl.when(n == N - 1)
        def _():
            z_whole(n - 1).wait_recv()
            join(zr.at[n - 1], COLS // TILE, 0)

            def put(t, _):
                out[:, tile(t)] = pt[slot, y, tile(t), :].T
                return 0

            lax.fori_loop(0, COLS // TILE, put, 0)

    def step(it, _):
        @pl.when(it < N)
        def _():
            a(it)

        @pl.when(it == 0)
        def _():
            x1(1)

        @pl.when(it < N - 3)
        def _():
            x0(it + 3)

        @pl.when(it < N - 2)
        def _():
            x1(it + 2)

        @pl.when((it >= 1) & (it < N + 1))
        def _():
            b(it - 1)

        @pl.when(it < N - 1)
        def _():
            x2(it + 1)

        @pl.when(it >= 2)
        def _():
            c(it - 2)

        return 0

    lax.fori_loop(0, N + 2, step, 0)

    for way, d in ways:
        for core in (0, 1):
            far_first(way, d, core).wait_send()
            far_second(way, d, core).wait_send()
        z_half(way, d).wait_send()
    for copy in nears:
        copy.wait_send()

    def drain(n, _):
        for copy in own_out(n) + first_out(n) + second_out(n):
            copy.wait_send()
        for i, hop in enumerate((1, -1, 2)):
            to_partner(n, hop, i).wait_send()
        relayed(n).wait_send()
        return 0

    lax.fori_loop(0, N, drain, 0)

    def drain_z(n, _):
        z_whole(n).wait_send()
        return 0

    lax.fori_loop(1, N - 1, drain_z, 0)


def local(features, cotangent):
    dma = pltpu.SemaphoreType.DMA
    return pl.pallas_call(
        kernel,
        out_shape=jax.ShapeDtypeStruct((BLK, COLS), f32),
        in_specs=[pl.BlockSpec(memory_space=pl.ANY)] * 2,
        out_specs=pl.BlockSpec(memory_space=pltpu.VMEM),
        scratch_shapes=[
            pltpu.VMEM((N, GROUP, CHUNK), bf16),
            pltpu.VMEM((GROUP, COLS), bf16),
            pltpu.VMEM((4, HALF, COLS), bf16),
            pltpu.VMEM((COLS, GROUP), bf16),
            pltpu.VMEM((4, NY, COLS, BLK), f32),
            pltpu.VMEM((N, 2, H + PAD, BLK), bf16),
            pltpu.VMEM((N, 2, H + PAD, BLK), bf16),
            pltpu.VMEM((N, 2, COLS + PAD, BLK), bf16),
            pltpu.VMEM((N, 2, COLS + PAD, BLK), bf16),
            pltpu.VMEM((N, COLS + PAD, BLK), bf16),
            pltpu.VMEM((N, COLS + PAD, BLK), bf16),
            dma((N,)), dma((1,)), dma((5,)), dma((8,)), dma((8,)), dma((4,)), dma((4,)),
            dma((N, 3)), dma((N, 3)), dma((N,)), dma((N, 8)),
            dma((N, 2)), dma((N, 2)), dma((N, 2)), dma((N, 2)), dma((N,)), dma((N,)),
        ],
        compiler_params=pltpu.CompilerParams(
            collective_id=0, has_side_effects=True, vmem_limit_bytes=62 * 1024 * 1024
        ),
        name="weight_grad",
    )(features, cotangent)


def solution(mesh):
    return jax.shard_map(
        local,
        mesh=mesh,
        in_specs=(P(("row", "col"), None), P(("row", "col"), None)),
        out_specs=P("row", "col"),
        check_vma=False,
    )
```

```python
import jax
import jax.numpy as jnp
from jax import lax
from jax.experimental import pallas as pl
from jax.experimental.pallas import tpu as pltpu
from jax.sharding import PartitionSpec as P

NX, NY, NZ = 4, 4, 8
TOK = 192
HALF = TOK // 2
GROUP = 8 * TOK
COLS = 1024
BLK = 128
CHUNK = NY * BLK
N = NZ
TILE = 32
WIDE = 128
LATE = 320
EARLY = COLS - LATE
H = EARLY // 2
L = LATE // 2

POWER = 32
LOW = 2.0**-3.9
SPAN = 2.0**3.9 - 2.0**-3.9
PAD = 16

f32, bf16 = jnp.float32, jnp.bfloat16


def rows(start, size):
    return pl.ds(pl.multiple_of(start, 32), size)


def tile(t):
    return pl.ds(pl.multiple_of(t * TILE, TILE), TILE)


def wide(t):
    return pl.ds(pl.multiple_of(t * WIDE, WIDE), WIDE)


def each(count, body):
    step = next(u for u in range(12, 0, -1) if count % u == 0)

    def group(g, _):
        for i in range(step):
            body(g * step + i)
        return 0

    if count == step:
        group(0, 0)
    else:
        lax.fori_loop(0, count // step, group, 0)


def encode(read, first, tiles, message):
    def widest(t, most):
        value = jnp.abs(read(first + t))
        return jnp.maximum(most, jnp.max(value.reshape(TILE // 8, 8, BLK), axis=0))

    most = jnp.zeros((8, BLK), f32)
    if tiles <= 12:
        for t in range(tiles):
            most = widest(t, most)
    else:
        most = lax.fori_loop(
            0, tiles // 2, lambda t, m: widest(2 * t + 1, widest(2 * t, m)), most
        )
    most = jnp.maximum(jnp.max(most, axis=0, keepdims=True) * 1.01, 1e-30)
    most = jnp.broadcast_to(most, (PAD, BLK)).astype(bf16)
    message[pl.ds(tiles * TILE, PAD), :] = most
    scale = SPAN / most.astype(f32)[:1]

    def code(t):
        value = read(first + t)
        power = jnp.abs(value) * scale + LOW
        for _ in range(5):
            power = power * power
        message[tile(t), :] = jnp.where(value < 0, -power, power).astype(bf16)

    each(tiles, code)


def decoder(message, tiles):
    scale = message[pl.ds(tiles * TILE, PAD), :].astype(f32)[:1] * (1.0 / SPAN)

    def decode(t):
        value = message[tile(t), :].astype(f32)
        root = jnp.exp2(jnp.log(jnp.abs(value)) * (1.4426950408889634 / POWER))
        size = (root - LOW) * scale
        return jnp.where(value < 0, -size, size)

    return decode


def kernel(
    f_in, c_in, out, f_all, c_all, relay, ct, pt, s1, r1, s2, r2, zs, zr,
    ws, wr, t1, u1, t2, u2,
    f_own, c_own, c_out, c_far_out, c_get, c_far, c_relay,
    f_out, f_pass, f_relay, f_get, f_far, y1_out, y1_get, y2_out, y2_get, z_out, z_get,
    w_out, w_get, t1_out, t1_get, t2_out, t2_get,
):
    row, col = lax.axis_index("row"), lax.axis_index("col")
    y, z = lax.div(row, NZ), lax.rem(row, NZ)
    x, k = lax.div(col, 2), lax.rem(col, 2)

    def on_x(step, core):
        return {"row": row, "col": lax.rem(x + step + NX, NX) * 2 + core}

    def on_y(step):
        return {"row": lax.rem(y + step + NY, NY) * NZ + z, "col": col}

    def on_z(step):
        return {"row": y * NZ + lax.rem(z + step + NZ, NZ), "col": col}

    def place(step, core):
        return lax.rem(x + step + NX, NX) * 2 + core

    def send(src, dst, out_sem, get_sem, to):
        return pltpu.make_async_remote_copy(
            src_ref=src, dst_ref=dst, send_sem=out_sem, recv_sem=get_sem,
            device_id=to, device_id_type=pl.DeviceIdType.MESH,
        )

    partner = on_x(0, 1 - k)

    def offset(n):
        far = N // 2 - lax.div(n + 1, 2)
        return lax.rem(z + far * (2 * lax.rem(n, 2) - 1) + NZ, NZ)

    def own_features(n, _):
        for yy in range(NY):
            at = pl.multiple_of((yy * NZ + offset(n)) * BLK, BLK)
            pltpu.make_async_copy(
                f_in.at[:, pl.ds(at, BLK)],
                f_all.at[n, rows(col * TOK, TOK), pl.ds(yy * BLK, BLK)],
                f_own.at[n],
            ).start()
        return 0

    def columns(device):
        return pl.ds(pl.multiple_of(device * COLS, COLS), COLS)

    lax.fori_loop(0, N, own_features, 0)
    keep = pltpu.make_async_copy(
        c_in.at[:, columns(col)], c_all.at[rows(col * TOK, TOK), :], c_own.at[0]
    )
    keep.start()

    barrier = pltpu.get_barrier_semaphore()
    peers = [partner] + [on_x(d, c) for d in (1, -1) for c in (0, 1)]
    peers += [on_y(1), on_y(-1), on_z(1), on_z(-1)]
    for peer in peers:
        pl.semaphore_signal(
            barrier, inc=1, device_id=peer, device_id_type=pl.DeviceIdType.MESH
        )
    pl.semaphore_wait(barrier, len(peers))

    ways = ((0, 1), (1, -1))

    def far_first(way, d, c):
        return send(
            c_in.at[pl.ds(way * HALF, HALF), columns(place(2, c))],
            relay.at[way * 2 + c], c_far_out.at[way * 2 + c], c_relay.at[way * 2 + c],
            on_x(d, k),
        )

    def far_second(way, d, c):
        at = rows(place(-d, k) * TOK + way * HALF, HALF)
        return send(
            relay.at[way * 2 + c], c_all.at[at, :],
            c_far_out.at[4 + way * 2 + c], c_far.at[way * 2 + k], on_x(d, c),
        )

    def near(step, c, slot):
        return send(
            c_in.at[:, columns(place(step, c))], c_all.at[rows(col * TOK, TOK), :],
            c_out.at[slot], c_get.at[col], on_x(step, c),
        )

    nears = [near(d, c, way * 2 + c) for way, d in ways for c in (0, 1)]
    nears.append(near(0, 1 - k, 4))
    for way, d in ways:
        for c in (0, 1):
            far_first(way, d, c).start()
    for copy in nears:
        copy.start()

    def block(n, device):
        return f_all.at[n, rows(device * TOK, TOK), :]

    def pass_on(n, device, out_sem, to):
        return send(block(n, device), block(n, device), out_sem, f_get.at[n, device], to)

    def own_out(n):
        return [
            pass_on(n, col, f_out.at[n, 0], on_x(1, k)),
            pass_on(n, col, f_out.at[n, 1], on_x(-1, k)),
            pass_on(n, col, f_out.at[n, 2], partner),
        ]

    def to_partner(n, step, slot):
        return pass_on(n, place(step, k), f_pass.at[n, slot], partner)

    def relayed(n):
        copies = []
        for i, d in ways:
            at = f_all.at[n, rows(place(-d, k) * TOK + i * HALF, HALF), :]
            copies.append(send(at, at, f_relay.at[n, i], f_far.at[n, i], on_x(d, k)))
        return copies

    def arrived(n, device):
        pass_on(n, device, f_out.at[n, 0], f_partner).wait_recv()

    f_partner = partner

    def x0(n):
        pltpu.make_async_copy(
            f_in.at[:, pl.ds(0, CHUNK)], block(n, col), f_own.at[n]
        ).wait()
        for copy in own_out(n):
            copy.start()

    def x1(n):
        arrived(n, place(1, k))
        arrived(n, place(-1, k))
        for copy in relayed(n):
            copy.start()
        to_partner(n, 1, 0).start()
        to_partner(n, -1, 1).start()

    def x2(n):
        for copy in relayed(n):
            copy.wait_recv()
        to_partner(n, 2, 2).start()

    x0(0)
    for way, d in ways:
        for c in (0, 1):
            far_first(way, d, c).wait_recv()
            far_second(way, d, c).start()
    x1(0)
    x0(1)
    x0(2)

    keep.wait()
    for step, c in ((0, 1 - k), (1, 0), (1, 1), (-1, 0), (-1, 1)):
        send(
            c_in.at[:, columns(0)], c_all.at[rows(0, TOK), :],
            c_out.at[0], c_get.at[place(step, c)], partner,
        ).wait_recv()
    for i in range(4):
        send(
            relay.at[i], c_all.at[rows(0, HALF), :], c_out.at[0], c_far.at[i], partner
        ).wait_recv()

    def transpose(t, _):
        ct[:, wide(t)] = c_all[wide(t), :].T
        return 0

    lax.fori_loop(0, GROUP // WIDE, transpose, 0)
    x2(0)

    y_up, y_down = lax.rem(y + 1, NY), lax.rem(y + 3, NY)
    y_far = lax.rem(y + 2, NY)

    def first_out(n):
        return [
            send(s1.at[n, i], r1.at[n, i], y1_out.at[n, i], y1_get.at[n, i], on_y(d))
            for i, d in ways
        ]

    def second_out(n):
        return [
            send(s2.at[n, i], r2.at[n, i], y2_out.at[n, i], y2_get.at[n, i], on_y(d))
            for i, d in ways
        ]

    def a(n):
        slot = lax.rem(n, 4)
        for c in range(NX):
            arrived(n, c * 2 + 1 - k)

        def product(m, _):
            at = pl.ds(pl.multiple_of(m * 256, 256), 256)
            value = jnp.dot(ct[at, :], f_all[n], preferred_element_type=f32)
            for yy in range(NY):
                pt[slot, yy, at, :] = value[:, yy * BLK : (yy + 1) * BLK]
            return 0

        lax.fori_loop(0, COLS // 256, product, 0)
        half = H // TILE
        for i in (0, 1):
            encode(lambda t: pt[slot, y_far, tile(t), :], i * half, half, s1.at[n, i])
        for copy in first_out(n):
            copy.start()

    def b(n):
        slot = lax.rem(n, 4)
        half = H // TILE
        arriving = first_out(n)
        leaving = second_out(n)
        for i, target in ((0, y_up), (1, y_down)):
            arriving[i].wait_recv()
            decode = decoder(r1.at[n, i], half)

            def add(t):
                at = tile(i * half + t)
                pt[slot, target, at, :] += decode(t)

            each(half, add)
            encode(lambda t: pt[slot, target, tile(t), :], 0, EARLY // TILE, s2.at[n, i])
            leaving[i].start()

    part = H + PAD

    def z_half(i, d):
        return send(
            zs.at[i * 7, pl.ds(0, part), :], zr.at[i * 7, pl.ds(0, part), :],
            z_out.at[i * 7], z_get.at[i * 7], on_z(d),
        )

    def z_whole(n):
        d = 2 * lax.rem(n, 2) - 1
        return send(zs.at[n], zr.at[n], z_out.at[n], z_get.at[n], on_z(d))

    def w_half(i, d, j):
        return send(
            ws.at[i * 7, j, pl.ds(0, L + PAD), :], wr.at[i * 7, j, pl.ds(0, L + PAD), :],
            w_out.at[i * 7, j], w_get.at[i * 7, j], on_z(d),
        )

    def w_whole(n, j):
        d = 2 * lax.rem(n, 2) - 1
        return send(ws.at[n, j], wr.at[n, j], w_out.at[n, j], w_get.at[n, j], on_z(d))

    def late_first(i, d):
        return send(t1.at[i], u1.at[i], t1_out.at[i], t1_get.at[i], on_y(d))

    def late_second(i, d):
        return send(t2.at[i], u2.at[i], t2_out.at[i], t2_get.at[i], on_y(d))

    base = EARLY // TILE

    order = (y_far, y_up, y_down, y)

    def late(n, which=range(NY)):
        slot = lax.rem(n, 4)

        def reader(yy):
            return lambda t: pt[slot, yy, tile(base + t), :]

        def join(slot_in, j, tiles, first):
            decode = decoder(wr.at[slot_in, j], tiles)

            def add(t):
                pt[slot, order[j], tile(base + first + t), :] += decode(t)

            each(tiles, add)

        half, full = L // TILE, LATE // TILE

        for j in which:

            @pl.when(n == 0)
            def _():
                for i, d in ways:
                    encode(reader(order[j]), i * half, half, ws.at[i * 7, j])
                    w_half(i, d, j).start()

            @pl.when(n == 1)
            def _():
                w_half(0, 1, j).wait_recv()
                join(0, j, half, 0)

            @pl.when(n == 2)
            def _():
                w_half(1, -1, j).wait_recv()
                join(7, j, half, half)

            @pl.when(n >= 3)
            def _():
                w_whole(n - 2, j).wait_recv()
                join(n - 2, j, full, 0)

            @pl.when((n >= 1) & (n < N - 1))
            def _():
                encode(reader(order[j]), 0, full, ws.at[n, j])
                w_whole(n, j).start()

            @pl.when(n == N - 1)
            def _():
                w_whole(n - 1, j).wait_recv()
                join(n - 1, j, full, 0)
                if j == 0:
                    for i, d in ways:
                        encode(reader(y_far), i * half, half, t1.at[i])
                        late_first(i, d).start()

    last = (N - 1) % 4

    def late_middle():
        for i, d in ways:
            target = (y_up, y_down)[i]
            late_first(i, d).wait_recv()
            decode = decoder(u1.at[i], L // TILE)
            for t in range(L // TILE):
                pt[last, target, tile(base + i * (L // TILE) + t), :] += decode(t)
            encode(lambda t: pt[last, target, tile(base + t), :], 0, LATE // TILE, t2.at[i])
            late_second(i, d).start()

    def late_end():
        for i, d in ways:
            late_second(i, d).wait_recv()
            decode = decoder(u2.at[i], LATE // TILE)
            for t in range(LATE // TILE):
                pt[last, y, tile(base + t), :] += decode(t)

    def c(n):
        slot = lax.rem(n, 4)
        half = H // TILE
        arriving = second_out(n)
        arriving[0].wait_recv()
        arriving[1].wait_recv()
        up = decoder(r2.at[n, 0], EARLY // TILE)
        down = decoder(r2.at[n, 1], EARLY // TILE)

        def total(t):
            pt[slot, y, tile(t), :] += up(t) + down(t)

        each(EARLY // TILE, total)

        def read(t):
            return pt[slot, y, tile(t), :]

        def join(message, tiles, first):
            decode = decoder(message, tiles)

            def add(t):
                pt[slot, y, tile(first + t), :] += decode(t)

            each(tiles, add)

        @pl.when(n == 0)
        def _():
            for i, d in ways:
                encode(read, i * half, half, zs.at[i * 7])
                z_half(i, d).start()

        @pl.when(n == 1)
        def _():
            z_half(0, 1).wait_recv()
            join(zr.at[0], half, 0)

        @pl.when(n == 2)
        def _():
            z_half(1, -1).wait_recv()
            join(zr.at[7], half, half)

        @pl.when(n >= 3)
        def _():
            z_whole(n - 2).wait_recv()
            join(zr.at[n - 2], EARLY // TILE, 0)

        @pl.when((n >= 1) & (n < N - 1))
        def _():
            encode(read, 0, EARLY // TILE, zs.at[n])
            z_whole(n).start()

        @pl.when(n == N - 1)
        def _():
            z_whole(n - 1).wait_recv()
            join(zr.at[n - 1], EARLY // TILE, 0)
            late_end()

            def put(t, _):
                out[:, wide(t)] = pt[slot, y, wide(t), :].T
                return 0

            lax.fori_loop(0, COLS // WIDE, put, 0)

    def step(it, _):
        @pl.when(it < N)
        def _():
            a(it)

        @pl.when(it == N - 1)
        def _():
            late(N - 1, (0,))

        @pl.when(it == 0)
        def _():
            x1(1)
            x0(3)

        @pl.when((it >= 1) & (it < N + 1))
        def _():
            b(it - 1)

        @pl.when(it < N - 2)
        def _():
            x1(it + 2)

        @pl.when(it < N - 4)
        def _():
            x0(it + 4)

        @pl.when(it < N - 1)
        def _():
            x2(it + 1)
            late(it)

        @pl.when(it == N)
        def _():
            late(N - 1, (1, 2, 3))
            late_middle()

        @pl.when(it >= 2)
        def _():
            c(it - 2)

        return 0

    lax.fori_loop(0, N + 2, step, 0)

    for way, d in ways:
        for core in (0, 1):
            far_first(way, d, core).wait_send()
            far_second(way, d, core).wait_send()
        z_half(way, d).wait_send()
        for j in range(NY):
            w_half(way, d, j).wait_send()
        late_first(way, d).wait_send()
        late_second(way, d).wait_send()
    for copy in nears:
        copy.wait_send()

    def drain(n, _):
        for copy in own_out(n) + relayed(n) + first_out(n) + second_out(n):
            copy.wait_send()
        for i, hop in enumerate((1, -1, 2)):
            to_partner(n, hop, i).wait_send()
        return 0

    lax.fori_loop(0, N, drain, 0)

    def drain_z(n, _):
        z_whole(n).wait_send()
        for j in range(NY):
            w_whole(n, j).wait_send()
        return 0

    lax.fori_loop(1, N - 1, drain_z, 0)


def local(features, cotangent):
    dma = pltpu.SemaphoreType.DMA
    return pl.pallas_call(
        kernel,
        out_shape=pltpu.VMEM((BLK, COLS), f32),
        in_specs=[pl.BlockSpec(memory_space=pl.ANY)] * 2,
        out_specs=pl.BlockSpec(memory_space=pltpu.VMEM),
        scratch_shapes=[
            pltpu.VMEM((N, GROUP, CHUNK), bf16),
            pltpu.VMEM((GROUP, COLS), bf16),
            pltpu.VMEM((4, HALF, COLS), bf16),
            pltpu.VMEM((COLS, GROUP), bf16),
            pltpu.VMEM((4, NY, COLS, BLK), f32),
            pltpu.VMEM((N, 2, H + PAD, BLK), bf16),
            pltpu.VMEM((N, 2, H + PAD, BLK), bf16),
            pltpu.VMEM((N, 2, EARLY + PAD, BLK), bf16),
            pltpu.VMEM((N, 2, EARLY + PAD, BLK), bf16),
            pltpu.VMEM((N, EARLY + PAD, BLK), bf16),
            pltpu.VMEM((N, EARLY + PAD, BLK), bf16),
            pltpu.VMEM((N, NY, LATE + PAD, BLK), bf16),
            pltpu.VMEM((N, NY, LATE + PAD, BLK), bf16),
            pltpu.VMEM((2, L + PAD, BLK), bf16),
            pltpu.VMEM((2, L + PAD, BLK), bf16),
            pltpu.VMEM((2, LATE + PAD, BLK), bf16),
            pltpu.VMEM((2, LATE + PAD, BLK), bf16),
            dma((N,)), dma((1,)), dma((5,)), dma((8,)), dma((8,)), dma((4,)), dma((4,)),
            dma((N, 3)), dma((N, 3)), dma((N, 2)), dma((N, 8)), dma((N, 2)),
            dma((N, 2)), dma((N, 2)), dma((N, 2)), dma((N, 2)), dma((N,)), dma((N,)),
            dma((N, NY)), dma((N, NY)), dma((2,)), dma((2,)), dma((2,)), dma((2,)),
        ],
        compiler_params=pltpu.CompilerParams(
            collective_id=0, has_side_effects=True, vmem_limit_bytes=62 * 1024 * 1024
        ),
        name="weight_grad",
    )(features, cotangent)


def solution(mesh):
    return jax.shard_map(
        local,
        mesh=mesh,
        in_specs=(P(("row", "col"), None), P(("row", "col"), None)),
        out_specs=P("row", "col"),
        check_vma=False,
    )
```

```python
import jax
import jax.numpy as jnp
from jax import lax
from jax.experimental import pallas as pl
from jax.experimental.pallas import tpu as pltpu
from jax.sharding import PartitionSpec as P

NX, NY, NZ = 4, 4, 8
TOK = 192
HALF = TOK // 2
GROUP = 8 * TOK
COLS = 1024
BLK = 128
CHUNK = NY * BLK
N = NZ
TILE = 32
WIDE = 128
LATE = 384
EARLY = COLS - LATE
H = EARLY // 2
L = LATE // 2

POWER = 32
LOW = 2.0**-3.9
SPAN = 2.0**3.9 - 2.0**-3.9
PAD = 16

f32, bf16 = jnp.float32, jnp.bfloat16


def rows(start, size):
    return pl.ds(pl.multiple_of(start, 32), size)


def tile(t):
    return pl.ds(pl.multiple_of(t * TILE, TILE), TILE)


def wide(t):
    return pl.ds(pl.multiple_of(t * WIDE, WIDE), WIDE)


def each(count, body):
    step = next(u for u in range(12, 0, -1) if count % u == 0)

    def group(g, _):
        for i in range(step):
            body(g * step + i)
        return 0

    if count == step:
        group(0, 0)
    else:
        lax.fori_loop(0, count // step, group, 0)


def encode(read, first, tiles, message):
    def widest(t, most):
        value = jnp.abs(read(first + t))
        return jnp.maximum(most, jnp.max(value.reshape(TILE // 8, 8, BLK), axis=0))

    most = jnp.zeros((8, BLK), f32)
    if tiles <= 12:
        for t in range(tiles):
            most = widest(t, most)
    else:
        most = lax.fori_loop(
            0, tiles // 2, lambda t, m: widest(2 * t + 1, widest(2 * t, m)), most
        )
    most = jnp.maximum(jnp.max(most, axis=0, keepdims=True) * 1.01, 1e-30)
    most = jnp.broadcast_to(most, (PAD, BLK)).astype(bf16)
    message[pl.ds(tiles * TILE, PAD), :] = most
    scale = SPAN / most.astype(f32)[:1]

    def code(t):
        value = read(first + t)
        power = jnp.abs(value) * scale + LOW
        for _ in range(5):
            power = power * power
        message[tile(t), :] = jnp.where(value < 0, -power, power).astype(bf16)

    each(tiles, code)


def decoder(message, tiles):
    scale = message[pl.ds(tiles * TILE, PAD), :].astype(f32)[:1] * (1.0 / SPAN)

    def decode(t):
        value = message[tile(t), :].astype(f32)
        root = jnp.exp2(jnp.log(jnp.abs(value)) * (1.4426950408889634 / POWER))
        size = (root - LOW) * scale
        return jnp.where(value < 0, -size, size)

    return decode


def kernel(
    f_in, c_in, out, f_all, c_all, relay, ct, pt, s1, r1, s2, r2, zs, zr,
    ws, wr, t1, u1, t2, u2,
    f_own, c_own, c_out, c_relay, c_get, f_send, f_near, f_far, f_mate,
    y1_out, y1_get, y2_out, y2_get, z_out, z_get, w_out, w_get,
    t1_out, t1_get, t2_out, t2_get,
):
    row, col = lax.axis_index("row"), lax.axis_index("col")
    y, z = lax.div(row, NZ), lax.rem(row, NZ)
    x, k = lax.div(col, 2), lax.rem(col, 2)

    def on_x(step, core):
        return {"row": row, "col": lax.rem(x + step + NX, NX) * 2 + core}

    def on_y(step):
        return {"row": lax.rem(y + step + NY, NY) * NZ + z, "col": col}

    def on_z(step):
        return {"row": y * NZ + lax.rem(z + step + NZ, NZ), "col": col}

    def place(step, core):
        return lax.rem(x + step + NX, NX) * 2 + core

    def send(src, dst, out_sem, get_sem, to):
        return pltpu.make_async_remote_copy(
            src_ref=src, dst_ref=dst, send_sem=out_sem, recv_sem=get_sem,
            device_id=to, device_id_type=pl.DeviceIdType.MESH,
        )

    partner = on_x(0, 1 - k)

    def left(ref, sem):
        send(ref, ref, sem, c_get.at[0], partner).wait_send()

    def landed(ref, sem):
        send(ref, ref, c_out.at[0], sem, partner).wait_recv()

    FAR, UP, DOWN, OWN = range(NY)
    order = (lax.rem(y + 2, NY), lax.rem(y + 1, NY), lax.rem(y + 3, NY), y)

    def offset(n):
        far = N // 2 - lax.div(n + 1, 2)
        return lax.rem(z + far * (2 * lax.rem(n, 2) - 1) + NZ, NZ)

    def own_features(n, _):
        for j in range(NY):
            at = pl.multiple_of((order[j] * NZ + offset(n)) * BLK, BLK)
            pltpu.make_async_copy(
                f_in.at[:, pl.ds(at, BLK)],
                f_all.at[n, rows(col * TOK, TOK), pl.ds(j * BLK, BLK)],
                f_own.at[n],
            ).start()
        return 0

    def columns(device):
        return pl.ds(pl.multiple_of(device * COLS, COLS), COLS)

    lax.fori_loop(0, N, own_features, 0)
    keep = pltpu.make_async_copy(
        c_in.at[:, columns(col)], c_all.at[rows(col * TOK, TOK), :], c_own.at[0]
    )
    keep.start()

    barrier = pltpu.get_barrier_semaphore()
    peers = [partner] + [on_x(d, c) for d in (1, -1) for c in (0, 1)]
    peers += [on_y(1), on_y(-1), on_z(1), on_z(-1)]
    for peer in peers:
        pl.semaphore_signal(
            barrier, inc=1, device_id=peer, device_id_type=pl.DeviceIdType.MESH
        )
    pl.semaphore_wait(barrier, len(peers))

    ways = ((0, 1), (1, -1))

    def far_first(way, d, c):
        return send(
            c_in.at[pl.ds(way * HALF, HALF), columns(place(2, c))],
            relay.at[way * 2 + c], c_out.at[1], c_relay.at[way * 2 + c],
            on_x(d, k),
        )

    def far_second(way, d, c):
        at = rows(place(-d, k) * TOK + way * HALF, HALF)
        return send(
            relay.at[way * 2 + c], c_all.at[at, :], c_out.at[1], c_get.at[0], on_x(d, c),
        )

    def near(step, c):
        return send(
            c_in.at[:, columns(place(step, c))], c_all.at[rows(col * TOK, TOK), :],
            c_out.at[0], c_get.at[0], on_x(step, c),
        )

    nears = [near(d, c) for _, d in ways for c in (0, 1)]
    nears.append(near(0, 1 - k))
    for way, d in ways:
        for c in (0, 1):
            far_first(way, d, c).start()
    for copy in nears:
        copy.start()

    def block(n, device):
        return f_all.at[n, rows(device * TOK, TOK), :]

    def pass_on(n, device, out_sem, get_sem, to):
        return send(block(n, device), block(n, device), out_sem, get_sem, to)

    def own_out(n):
        return [
            pass_on(n, col, f_send.at[0], f_near.at[n], on_x(1, k)),
            pass_on(n, col, f_send.at[0], f_near.at[n], on_x(-1, k)),
            pass_on(n, col, f_send.at[0], f_mate.at[n], partner),
        ]

    def to_partner(n, step):
        return pass_on(n, place(step, k), f_send.at[1], f_mate.at[n], partner)

    def relayed(n):
        copies = []
        for i, d in ways:
            at = f_all.at[n, rows(place(-d, k) * TOK + i * HALF, HALF), :]
            copies.append(send(at, at, f_send.at[2], f_far.at[n], on_x(d, k)))
        return copies

    def blocks(n, count):
        return f_all.at[n, pl.ds(0, count * TOK), :]

    def x0(n):
        pltpu.make_async_copy(
            f_in.at[:, pl.ds(0, CHUNK)], block(n, col), f_own.at[n]
        ).wait()
        for copy in own_out(n):
            copy.start()

    def x1(n):
        landed(blocks(n, 2), f_near.at[n])
        for copy in relayed(n):
            copy.start()
        to_partner(n, 1).start()
        to_partner(n, -1).start()

    def x2(n):
        landed(blocks(n, 1), f_far.at[n])
        to_partner(n, 2).start()

    x0(0)
    for way, d in ways:
        for c in (0, 1):
            far_first(way, d, c).wait_recv()
            far_second(way, d, c).start()
    x1(0)
    x0(1)
    x0(2)

    keep.wait()
    landed(c_all.at[pl.ds(0, 7 * TOK), :], c_get.at[0])

    def transpose(t, _):
        ct[:, wide(t)] = c_all[wide(t), :].T
        return 0

    lax.fori_loop(0, GROUP // WIDE, transpose, 0)
    x2(0)

    def first_out(n):
        return [
            send(s1.at[n, i], r1.at[n, i], y1_out.at[0], y1_get.at[n, i], on_y(d))
            for i, d in ways
        ]

    def second_out(n):
        return [
            send(s2.at[n, i], r2.at[n, i], y2_out.at[0], y2_get.at[n], on_y(d))
            for i, d in ways
        ]

    def a(n):
        slot = lax.rem(n, 4)
        landed(blocks(n, 4), f_mate.at[n])

        value = jnp.dot(ct[...], f_all[n], preferred_element_type=f32)
        for j in range(NY):
            pt[slot, j] = value[:, j * BLK : (j + 1) * BLK]
        half = H // TILE
        for i in (0, 1):
            encode(lambda t: pt[slot, FAR, tile(t), :], i * half, half, s1.at[n, i])
        for copy in first_out(n):
            copy.start()

    def b(n):
        slot = lax.rem(n, 4)
        half = H // TILE
        arriving = first_out(n)
        leaving = second_out(n)
        for i, target in ((0, UP), (1, DOWN)):
            arriving[i].wait_recv()
            decode = decoder(r1.at[n, i], half)

            def add(t):
                at = tile(i * half + t)
                pt[slot, target, at, :] += decode(t)

            each(half, add)
            encode(lambda t: pt[slot, target, tile(t), :], 0, EARLY // TILE, s2.at[n, i])
            leaving[i].start()

    part = H + PAD

    def z_half(i, d):
        return send(
            zs.at[i * 7, pl.ds(0, part), :], zr.at[i * 7, pl.ds(0, part), :],
            z_out.at[1], z_get.at[i * 7], on_z(d),
        )

    def z_whole(n):
        d = 2 * lax.rem(n, 2) - 1
        return send(zs.at[n], zr.at[n], z_out.at[0], z_get.at[n], on_z(d))

    def w_half(i, d, j):
        return send(
            ws.at[i * 7, j, pl.ds(0, L + PAD), :], wr.at[i * 7, j, pl.ds(0, L + PAD), :],
            w_out.at[1], w_get.at[i * 7, j], on_z(d),
        )

    def w_whole(n, j):
        d = 2 * lax.rem(n, 2) - 1
        return send(ws.at[n, j], wr.at[n, j], w_out.at[0], w_get.at[n, j], on_z(d))

    def late_first(i, d):
        return send(t1.at[i], u1.at[i], t1_out.at[0], t1_get.at[i], on_y(d))

    def late_second(i, d):
        return send(t2.at[i], u2.at[i], t2_out.at[0], t2_get.at[i], on_y(d))

    base = EARLY // TILE

    def late(n, which=range(NY)):
        slot = lax.rem(n, 4)

        def reader(j):
            return lambda t: pt[slot, j, tile(base + t), :]

        def join(slot_in, j, tiles, first):
            decode = decoder(wr.at[slot_in, j], tiles)

            def add(t):
                pt[slot, j, tile(base + first + t), :] += decode(t)

            each(tiles, add)

        half, full = L // TILE, LATE // TILE

        for j in which:

            @pl.when(n == 0)
            def _():
                for i, d in ways:
                    encode(reader(j), i * half, half, ws.at[i * 7, j])
                    w_half(i, d, j).start()

            @pl.when(n == 1)
            def _():
                w_half(0, 1, j).wait_recv()
                join(0, j, half, 0)

            @pl.when(n == 2)
            def _():
                w_half(1, -1, j).wait_recv()
                join(7, j, half, half)

            @pl.when(n >= 3)
            def _():
                w_whole(n - 2, j).wait_recv()
                join(n - 2, j, full, 0)

            @pl.when((n >= 1) & (n < N - 1))
            def _():
                encode(reader(j), 0, full, ws.at[n, j])
                w_whole(n, j).start()

            @pl.when(n == N - 1)
            def _():
                w_whole(n - 1, j).wait_recv()
                join(n - 1, j, full, 0)
                if j == 0:
                    for i, d in ways:
                        encode(reader(FAR), i * half, half, t1.at[i])
                        late_first(i, d).start()

    last = (N - 1) % 4

    def late_middle():
        for i, d in ways:
            target = (UP, DOWN)[i]
            late_first(i, d).wait_recv()
            decode = decoder(u1.at[i], L // TILE)
            for t in range(L // TILE):
                pt[last, target, tile(base + i * (L // TILE) + t), :] += decode(t)
            encode(lambda t: pt[last, target, tile(base + t), :], 0, LATE // TILE, t2.at[i])
            late_second(i, d).start()

    def late_end():
        for i, d in ways:
            late_second(i, d).wait_recv()
            decode = decoder(u2.at[i], LATE // TILE)
            for t in range(LATE // TILE):
                pt[last, OWN, tile(base + t), :] += decode(t)

    def c(n):
        slot = lax.rem(n, 4)
        half = H // TILE
        landed(r2.at[n], y2_get.at[n])
        up = decoder(r2.at[n, 0], EARLY // TILE)
        down = decoder(r2.at[n, 1], EARLY // TILE)

        def total(t):
            pt[slot, OWN, tile(t), :] += up(t) + down(t)

        each(EARLY // TILE, total)

        def read(t):
            return pt[slot, OWN, tile(t), :]

        def join(message, tiles, first):
            decode = decoder(message, tiles)

            def add(t):
                pt[slot, OWN, tile(first + t), :] += decode(t)

            each(tiles, add)

        @pl.when(n == 0)
        def _():
            for i, d in ways:
                encode(read, i * half, half, zs.at[i * 7])
                z_half(i, d).start()

        @pl.when(n == 1)
        def _():
            z_half(0, 1).wait_recv()
            join(zr.at[0], half, 0)

        @pl.when(n == 2)
        def _():
            z_half(1, -1).wait_recv()
            join(zr.at[7], half, half)

        @pl.when(n >= 3)
        def _():
            z_whole(n - 2).wait_recv()
            join(zr.at[n - 2], EARLY // TILE, 0)

        @pl.when((n >= 1) & (n < N - 1))
        def _():
            encode(read, 0, EARLY // TILE, zs.at[n])
            z_whole(n).start()

        @pl.when(n == N - 1)
        def _():
            z_whole(n - 1).wait_recv()
            join(zr.at[n - 1], EARLY // TILE, 0)
            late_end()

            def put(t, _):
                out[:, wide(t)] = pt[slot, OWN, wide(t), :].T
                return 0

            lax.fori_loop(0, COLS // WIDE, put, 0)

    def step(it, _):
        @pl.when(it < N)
        def _():
            a(it)

        @pl.when(it == N - 1)
        def _():
            late(N - 1, (0,))

        @pl.when(it == 0)
        def _():
            x1(1)
            x0(3)

        @pl.when((it >= 2) & (it < N + 1))
        def _():
            b(it - 1)

        @pl.when(it < N - 2)
        def _():
            x1(it + 2)

        @pl.when(it < N - 4)
        def _():
            x0(it + 4)

        @pl.when((it >= 3) & (it < N))
        def _():
            c(it - 3)

        @pl.when(it < N - 1)
        def _():
            x2(it + 1)
            late(it)

        @pl.when(it == 0)
        def _():
            b(0)

        @pl.when(it == N)
        def _():
            late(N - 1, (1, 2, 3))
            late_middle()
            c(N - 3)

        @pl.when(it >= N)
        def _():
            c(it - 2)

        return 0

    lax.fori_loop(0, N + 2, step, 0)

    left(c_all.at[pl.ds(0, 5 * TOK), :], c_out.at[0])
    left(c_all.at[pl.ds(0, 4 * TOK), :], c_out.at[1])
    left(f_all.at[pl.ds(0, 3)], f_send.at[0])
    left(f_all.at[pl.ds(0, 3)], f_send.at[1])
    left(f_all.at[0], f_send.at[2])
    left(s1, y1_out.at[0])
    left(s2, y2_out.at[0])
    left(zs.at[pl.ds(1, N - 2)], z_out.at[0])
    left(s1.at[0], z_out.at[1])
    left(ws.at[pl.ds(1, N - 2)], w_out.at[0])
    left(ws.at[pl.ds(0, 2), :, pl.ds(0, L + PAD), :], w_out.at[1])
    left(t1, t1_out.at[0])
    left(t2, t2_out.at[0])


def local(features, cotangent):
    dma = pltpu.SemaphoreType.DMA
    return pl.pallas_call(
        kernel,
        out_shape=pltpu.VMEM((BLK, COLS), f32),
        in_specs=[pl.BlockSpec(memory_space=pl.ANY)] * 2,
        out_specs=pl.BlockSpec(memory_space=pltpu.VMEM),
        scratch_shapes=[
            pltpu.VMEM((N, GROUP, CHUNK), bf16),
            pltpu.VMEM((GROUP, COLS), bf16),
            pltpu.VMEM((4, HALF, COLS), bf16),
            pltpu.VMEM((COLS, GROUP), bf16),
            pltpu.VMEM((4, NY, COLS, BLK), f32),
            pltpu.VMEM((N, 2, H + PAD, BLK), bf16),
            pltpu.VMEM((N, 2, H + PAD, BLK), bf16),
            pltpu.VMEM((N, 2, EARLY + PAD, BLK), bf16),
            pltpu.VMEM((N, 2, EARLY + PAD, BLK), bf16),
            pltpu.VMEM((N, EARLY + PAD, BLK), bf16),
            pltpu.VMEM((N, EARLY + PAD, BLK), bf16),
            pltpu.VMEM((N, NY, LATE + PAD, BLK), bf16),
            pltpu.VMEM((N, NY, LATE + PAD, BLK), bf16),
            pltpu.VMEM((2, L + PAD, BLK), bf16),
            pltpu.VMEM((2, L + PAD, BLK), bf16),
            pltpu.VMEM((2, LATE + PAD, BLK), bf16),
            pltpu.VMEM((2, LATE + PAD, BLK), bf16),
            dma((N,)), dma((1,)), dma((2,)), dma((4,)), dma((1,)), dma((3,)), dma((N,)),
            dma((N,)), dma((N,)), dma((1,)), dma((N, 2)), dma((1,)), dma((N,)), dma((2,)),
            dma((N,)), dma((2,)), dma((N, NY)), dma((1,)), dma((2,)), dma((1,)), dma((2,)),
        ],
        compiler_params=pltpu.CompilerParams(
            collective_id=0, has_side_effects=True, vmem_limit_bytes=62 * 1024 * 1024
        ),
        name="weight_grad",
    )(features, cotangent)


def solution(mesh):
    return jax.shard_map(
        local,
        mesh=mesh,
        in_specs=(P(("row", "col"), None), P(("row", "col"), None)),
        out_specs=P("row", "col"),
        check_vma=False,
    )
```

```python
import jax
import jax.numpy as jnp
from jax import lax
from jax.experimental import pallas as pl
from jax.experimental.pallas import tpu as pltpu
from jax.sharding import PartitionSpec as P

NX, NY, NZ = 4, 4, 8
TOK = 192
HALF = TOK // 2
GROUP = 8 * TOK
COLS = 1024
BLK = 128
CHUNK = NY * BLK
N = NZ
TILE = 32
WIDE = 128
LATE = 384
EARLY = COLS - LATE
H = EARLY // 2
L = LATE // 2

POWER = 32
LOW = 2.0**-3.9
SPAN = 2.0**3.9 - 2.0**-3.9
PAD = 16

f32, bf16 = jnp.float32, jnp.bfloat16


def rows(start, size):
    return pl.ds(pl.multiple_of(start, 32), size)


def tile(t):
    return pl.ds(pl.multiple_of(t * TILE, TILE), TILE)


def wide(t):
    return pl.ds(pl.multiple_of(t * WIDE, WIDE), WIDE)


def each(count, body):
    step = next(u for u in range(12, 0, -1) if count % u == 0)

    def group(g, _):
        for i in range(step):
            body(g * step + i)
        return 0

    if count == step:
        group(0, 0)
    else:
        lax.fori_loop(0, count // step, group, 0)


def encode(read, first, tiles, message):
    def widest(t, most):
        value = jnp.abs(read(first + t))
        return jnp.maximum(most, jnp.max(value.reshape(TILE // 8, 8, BLK), axis=0))

    most = jnp.zeros((8, BLK), f32)
    if tiles <= 12:
        for t in range(tiles):
            most = widest(t, most)
    else:
        most = lax.fori_loop(
            0, tiles // 2, lambda t, m: widest(2 * t + 1, widest(2 * t, m)), most
        )
    most = jnp.maximum(jnp.max(most, axis=0, keepdims=True) * 1.01, 1e-30)
    most = jnp.broadcast_to(most, (PAD, BLK)).astype(bf16)
    message[pl.ds(tiles * TILE, PAD), :] = most
    scale = SPAN / most.astype(f32)[:1]

    def code(t):
        value = read(first + t)
        power = jnp.abs(value) * scale + LOW
        for _ in range(5):
            power = power * power
        message[tile(t), :] = jnp.where(value < 0, -power, power).astype(bf16)

    each(tiles, code)


def decoder(message, tiles):
    scale = message[pl.ds(tiles * TILE, PAD), :].astype(f32)[:1] * (1.0 / SPAN)

    def decode(t):
        value = message[tile(t), :].astype(f32)
        root = jnp.exp2(jnp.log(jnp.abs(value)) * (1.4426950408889634 / POWER))
        size = (root - LOW) * scale
        return jnp.where(value < 0, -size, size)

    return decode


def kernel(
    f_in, c_in, out, f_all, c_all, relay, ct, pt, s1, r1, s2, r2, zs, zr,
    ws, wr, t1, u1, t2, u2,
    f_own, c_own, c_out, c_relay, c_get, f_send, f_near, f_far, f_mate,
    y1_out, y1_get, y2_out, y2_get, z_out, z_get, w_out, w_get,
    t1_out, t1_get, t2_out, t2_get,
):
    row, col = lax.axis_index("row"), lax.axis_index("col")
    y, z = lax.div(row, NZ), lax.rem(row, NZ)
    x, k = lax.div(col, 2), lax.rem(col, 2)

    def on_x(step, core):
        return {"row": row, "col": lax.rem(x + step + NX, NX) * 2 + core}

    def on_y(step):
        return {"row": lax.rem(y + step + NY, NY) * NZ + z, "col": col}

    def on_z(step):
        return {"row": y * NZ + lax.rem(z + step + NZ, NZ), "col": col}

    def place(step, core):
        return lax.rem(x + step + NX, NX) * 2 + core

    def send(src, dst, out_sem, get_sem, to):
        return pltpu.make_async_remote_copy(
            src_ref=src, dst_ref=dst, send_sem=out_sem, recv_sem=get_sem,
            device_id=to, device_id_type=pl.DeviceIdType.MESH,
        )

    partner = on_x(0, 1 - k)

    def left(ref, sem):
        send(ref, ref, sem, c_get.at[0], partner).wait_send()

    def landed(ref, sem):
        send(ref, ref, c_out.at[0], sem, partner).wait_recv()

    FAR, UP, DOWN, OWN = range(NY)
    order = (lax.rem(y + 2, NY), lax.rem(y + 1, NY), lax.rem(y + 3, NY), y)

    def offset(n):
        far = N // 2 - lax.div(n + 1, 2)
        return lax.rem(z + far * (2 * lax.rem(n, 2) - 1) + NZ, NZ)

    def own_features(n, _):
        for j in range(NY):
            at = pl.multiple_of((order[j] * NZ + offset(n)) * BLK, BLK)
            pltpu.make_async_copy(
                f_in.at[:, pl.ds(at, BLK)],
                f_all.at[n, rows(col * TOK, TOK), pl.ds(j * BLK, BLK)],
                f_own.at[n],
            ).start()
        return 0

    def columns(device):
        return pl.ds(pl.multiple_of(device * COLS, COLS), COLS)

    lax.fori_loop(0, N, own_features, 0)
    keep = pltpu.make_async_copy(
        c_in.at[:, columns(col)], c_all.at[rows(col * TOK, TOK), :], c_own.at[0]
    )
    keep.start()

    barrier = pltpu.get_barrier_semaphore()
    peers = [partner] + [on_x(d, c) for d in (1, -1) for c in (0, 1)]
    peers += [on_y(1), on_y(-1), on_z(1), on_z(-1)]
    for peer in peers:
        pl.semaphore_signal(
            barrier, inc=1, device_id=peer, device_id_type=pl.DeviceIdType.MESH
        )
    pl.semaphore_wait(barrier, len(peers))

    ways = ((0, 1), (1, -1))

    cuts = ((0, EARLY), (EARLY, LATE))

    def piece(device, p):
        start, size = cuts[p]
        return pl.ds(pl.multiple_of(device * COLS + start, WIDE), size)

    def cut(p):
        return pl.ds(cuts[p][0], cuts[p][1])

    def far_first(p, way, d, c):
        i = way * 2 + c
        return send(
            c_in.at[pl.ds(way * HALF, HALF), piece(place(2, c), p)],
            relay.at[i, :, cut(p)], c_out.at[1], c_relay.at[p, i], on_x(d, k),
        )

    def far_second(p, way, d, c):
        at = rows(place(-d, k) * TOK + way * HALF, HALF)
        return send(
            relay.at[way * 2 + c, :, cut(p)], c_all.at[at, cut(p)],
            c_out.at[1], c_get.at[p], on_x(d, c),
        )

    def near(p, step, c):
        return send(
            c_in.at[:, piece(place(step, c), p)], c_all.at[rows(col * TOK, TOK), cut(p)],
            c_out.at[0], c_get.at[p], on_x(step, c),
        )

    def far_start(p):
        for way, d in ways:
            for c in (0, 1):
                far_first(p, way, d, c).start()

    def near_start(p):
        for _, d in ways:
            for c in (0, 1):
                near(p, d, c).start()
        near(p, 0, 1 - k).start()

    def far_on(p):
        for way, d in ways:
            for c in (0, 1):
                far_first(p, way, d, c).wait_recv()
                far_second(p, way, d, c).start()

    def block(n, device):
        return f_all.at[n, rows(device * TOK, TOK), :]

    def pass_on(n, device, out_sem, get_sem, to):
        return send(block(n, device), block(n, device), out_sem, get_sem, to)

    def own_out(n):
        return [
            pass_on(n, col, f_send.at[0], f_near.at[n], on_x(1, k)),
            pass_on(n, col, f_send.at[0], f_near.at[n], on_x(-1, k)),
            pass_on(n, col, f_send.at[0], f_mate.at[n], partner),
        ]

    def to_partner(n, step):
        return pass_on(n, place(step, k), f_send.at[1], f_mate.at[n], partner)

    def relayed(n):
        copies = []
        for i, d in ways:
            at = f_all.at[n, rows(place(-d, k) * TOK + i * HALF, HALF), :]
            copies.append(send(at, at, f_send.at[2], f_far.at[n], on_x(d, k)))
        return copies

    def blocks(n, count):
        return f_all.at[n, pl.ds(0, count * TOK), :]

    def x0(n):
        pltpu.make_async_copy(
            f_in.at[:, pl.ds(0, CHUNK)], block(n, col), f_own.at[n]
        ).wait()
        for copy in own_out(n):
            copy.start()

    def x1(n):
        landed(blocks(n, 2), f_near.at[n])
        for copy in relayed(n):
            copy.start()
        to_partner(n, 1).start()
        to_partner(n, -1).start()

    def x2(n):
        landed(blocks(n, 1), f_far.at[n])
        to_partner(n, 2).start()

    def transpose(p):
        landed(c_all.at[pl.ds(0, 7 * TOK), cut(p)], c_get.at[p])

        def one(t, _):
            ct[cut(p), wide(t)] = c_all[wide(t), cut(p)].T
            return 0

        lax.fori_loop(0, GROUP // WIDE, one, 0)

    far_start(0)
    near_start(0)
    x0(0)
    far_on(0)
    x0(1)
    x1(0)
    far_start(1)
    x1(1)
    near_start(1)
    keep.wait()
    transpose(0)
    x2(0)
    far_on(1)
    x0(2)
    x0(3)

    def first_out(n):
        return [
            send(s1.at[n, i], r1.at[n, i], y1_out.at[0], y1_get.at[n, i], on_y(d))
            for i, d in ways
        ]

    def second_out(n):
        return [
            send(s2.at[n, i], r2.at[n, i], y2_out.at[0], y2_get.at[n], on_y(d))
            for i, d in ways
        ]

    def product(n, at):
        value = jnp.dot(ct[at, :], f_all[n], preferred_element_type=f32)
        for j in range(NY):
            pt[lax.rem(n, 4), j, at, :] = value[:, j * BLK : (j + 1) * BLK]

    def first(n):
        half = H // TILE
        for i in (0, 1):
            read = lambda t: pt[lax.rem(n, 4), FAR, tile(t), :]
            encode(read, i * half, half, s1.at[n, i])
        for copy in first_out(n):
            copy.start()

    def a(n):
        @pl.when(n >= 2)
        def _():
            landed(blocks(n, 4), f_mate.at[n])
            product(n, pl.ds(0, COLS))
            first(n)

        @pl.when(n < 2)
        def _():
            product(n, cut(1))

    def b(n):
        slot = lax.rem(n, 4)
        half = H // TILE
        arriving = first_out(n)
        leaving = second_out(n)
        for i, target in ((0, UP), (1, DOWN)):
            arriving[i].wait_recv()
            decode = decoder(r1.at[n, i], half)

            def add(t):
                at = tile(i * half + t)
                pt[slot, target, at, :] += decode(t)

            each(half, add)
            encode(lambda t: pt[slot, target, tile(t), :], 0, EARLY // TILE, s2.at[n, i])
            leaving[i].start()

    part = H + PAD

    def z_half(i, d):
        return send(
            zs.at[i * 7, pl.ds(0, part), :], zr.at[i * 7, pl.ds(0, part), :],
            z_out.at[1], z_get.at[i * 7], on_z(d),
        )

    def z_whole(n):
        d = 2 * lax.rem(n, 2) - 1
        return send(zs.at[n], zr.at[n], z_out.at[0], z_get.at[n], on_z(d))

    def w_half(i, d, j):
        return send(
            ws.at[i * 7, j, pl.ds(0, L + PAD), :], wr.at[i * 7, j, pl.ds(0, L + PAD), :],
            w_out.at[1], w_get.at[i * 7, j], on_z(d),
        )

    def w_whole(n, j):
        d = 2 * lax.rem(n, 2) - 1
        return send(ws.at[n, j], wr.at[n, j], w_out.at[0], w_get.at[n, j], on_z(d))

    def late_first(i, d):
        return send(t1.at[i], u1.at[i], t1_out.at[0], t1_get.at[i], on_y(d))

    def late_second(i, d):
        return send(t2.at[i], u2.at[i], t2_out.at[0], t2_get.at[i], on_y(d))

    base = EARLY // TILE

    def late(n, which=range(NY)):
        slot = lax.rem(n, 4)

        def reader(j):
            return lambda t: pt[slot, j, tile(base + t), :]

        def join(slot_in, j, tiles, first):
            decode = decoder(wr.at[slot_in, j], tiles)

            def add(t):
                pt[slot, j, tile(base + first + t), :] += decode(t)

            each(tiles, add)

        half, full = L // TILE, LATE // TILE

        for j in which:

            @pl.when(n == 0)
            def _():
                for i, d in ways:
                    encode(reader(j), i * half, half, ws.at[i * 7, j])
                    w_half(i, d, j).start()

            @pl.when(n == 1)
            def _():
                w_half(0, 1, j).wait_recv()
                join(0, j, half, 0)

            @pl.when(n == 2)
            def _():
                w_half(1, -1, j).wait_recv()
                join(7, j, half, half)

            @pl.when(n >= 3)
            def _():
                w_whole(n - 2, j).wait_recv()
                join(n - 2, j, full, 0)

            @pl.when((n >= 1) & (n < N - 1))
            def _():
                encode(reader(j), 0, full, ws.at[n, j])
                w_whole(n, j).start()

            @pl.when(n == N - 1)
            def _():
                w_whole(n - 1, j).wait_recv()
                join(n - 1, j, full, 0)
                if j == 0:
                    for i, d in ways:
                        encode(reader(FAR), i * half, half, t1.at[i])
                        late_first(i, d).start()

    def ahead(n):
        landed(blocks(n, 4), f_mate.at[n])
        product(n, cut(0))
        first(n)

    last = (N - 1) % 4

    def late_middle():
        for i, d in ways:
            target = (UP, DOWN)[i]
            late_first(i, d).wait_recv()
            decode = decoder(u1.at[i], L // TILE)
            for t in range(L // TILE):
                pt[last, target, tile(base + i * (L // TILE) + t), :] += decode(t)
            encode(lambda t: pt[last, target, tile(base + t), :], 0, LATE // TILE, t2.at[i])
            late_second(i, d).start()

    def late_end():
        for i, d in ways:
            late_second(i, d).wait_recv()
            decode = decoder(u2.at[i], LATE // TILE)
            for t in range(LATE // TILE):
                pt[last, OWN, tile(base + t), :] += decode(t)

    def c(n):
        slot = lax.rem(n, 4)
        half = H // TILE
        landed(r2.at[n], y2_get.at[n])
        up = decoder(r2.at[n, 0], EARLY // TILE)
        down = decoder(r2.at[n, 1], EARLY // TILE)

        def total(t):
            pt[slot, OWN, tile(t), :] += up(t) + down(t)

        each(EARLY // TILE, total)

        def read(t):
            return pt[slot, OWN, tile(t), :]

        def join(message, tiles, first):
            decode = decoder(message, tiles)

            def add(t):
                pt[slot, OWN, tile(first + t), :] += decode(t)

            each(tiles, add)

        @pl.when(n == 0)
        def _():
            for i, d in ways:
                encode(read, i * half, half, zs.at[i * 7])
                z_half(i, d).start()

        @pl.when(n == 1)
        def _():
            z_half(0, 1).wait_recv()
            join(zr.at[0], half, 0)

        @pl.when(n == 2)
        def _():
            z_half(1, -1).wait_recv()
            join(zr.at[7], half, half)

        @pl.when(n >= 3)
        def _():
            z_whole(n - 2).wait_recv()
            join(zr.at[n - 2], EARLY // TILE, 0)

        @pl.when((n >= 1) & (n < N - 1))
        def _():
            encode(read, 0, EARLY // TILE, zs.at[n])
            z_whole(n).start()

        @pl.when(n == N - 1)
        def _():
            z_whole(n - 1).wait_recv()
            join(zr.at[n - 1], EARLY // TILE, 0)
            late_end()

            def put(t, _):
                out[:, wide(t)] = pt[slot, OWN, wide(t), :].T
                return 0

            lax.fori_loop(0, COLS // WIDE, put, 0)

    def step(it, _):
        @pl.when(it < N)
        def _():
            a(it)

        @pl.when(it == N - 2)
        def _():
            late(N - 3)

        @pl.when(it == N - 1)
        def _():
            late(N - 1, (0,))

        @pl.when((it >= 2) & (it < N + 1))
        def _():
            b(it - 1)

        @pl.when(it < N - 2)
        def _():
            x1(it + 2)

        @pl.when(it < N - 4)
        def _():
            x0(it + 4)

        @pl.when((it >= 3) & (it < N))
        def _():
            c(it - 3)

        @pl.when((it >= 1) & (it < N - 1))
        def _():
            x2(it + 1)

        @pl.when((it < N - 1) & (it != N - 3))
        def _():
            late(it)

        @pl.when(it == N)
        def _():
            late(N - 1, (1, 2, 3))
            late_middle()
            c(N - 3)

        @pl.when(it >= N)
        def _():
            c(it - 2)

        return 0

    ahead(0)
    x2(1)
    ahead(1)
    b(0)
    transpose(1)
    lax.fori_loop(0, N + 2, step, 0)

    left(c_all.at[pl.ds(0, 5 * TOK), :], c_out.at[0])
    left(c_all.at[pl.ds(0, 4 * TOK), :], c_out.at[1])
    left(f_all.at[pl.ds(0, 3)], f_send.at[0])
    left(f_all.at[pl.ds(0, 3)], f_send.at[1])
    left(f_all.at[0], f_send.at[2])
    left(s1, y1_out.at[0])
    left(s2, y2_out.at[0])
    left(zs.at[pl.ds(1, N - 2)], z_out.at[0])
    left(s1.at[0], z_out.at[1])
    left(ws.at[pl.ds(1, N - 2)], w_out.at[0])
    left(ws.at[pl.ds(0, 2), :, pl.ds(0, L + PAD), :], w_out.at[1])
    left(t1, t1_out.at[0])
    left(t2, t2_out.at[0])


def local(features, cotangent):
    dma = pltpu.SemaphoreType.DMA
    return pl.pallas_call(
        kernel,
        out_shape=pltpu.VMEM((BLK, COLS), f32),
        in_specs=[pl.BlockSpec(memory_space=pl.ANY)] * 2,
        out_specs=pl.BlockSpec(memory_space=pltpu.VMEM),
        scratch_shapes=[
            pltpu.VMEM((N, GROUP, CHUNK), bf16),
            pltpu.VMEM((GROUP, COLS), bf16),
            pltpu.VMEM((4, HALF, COLS), bf16),
            pltpu.VMEM((COLS, GROUP), bf16),
            pltpu.VMEM((4, NY, COLS, BLK), f32),
            pltpu.VMEM((N, 2, H + PAD, BLK), bf16),
            pltpu.VMEM((N, 2, H + PAD, BLK), bf16),
            pltpu.VMEM((N, 2, EARLY + PAD, BLK), bf16),
            pltpu.VMEM((N, 2, EARLY + PAD, BLK), bf16),
            pltpu.VMEM((N, EARLY + PAD, BLK), bf16),
            pltpu.VMEM((N, EARLY + PAD, BLK), bf16),
            pltpu.VMEM((N, NY, LATE + PAD, BLK), bf16),
            pltpu.VMEM((N, NY, LATE + PAD, BLK), bf16),
            pltpu.VMEM((2, L + PAD, BLK), bf16),
            pltpu.VMEM((2, L + PAD, BLK), bf16),
            pltpu.VMEM((2, LATE + PAD, BLK), bf16),
            pltpu.VMEM((2, LATE + PAD, BLK), bf16),
            dma((N,)), dma((1,)), dma((2,)), dma((2, 4)), dma((2,)), dma((3,)), dma((N,)),
            dma((N,)), dma((N,)), dma((1,)), dma((N, 2)), dma((1,)), dma((N,)), dma((2,)),
            dma((N,)), dma((2,)), dma((N, NY)), dma((1,)), dma((2,)), dma((1,)), dma((2,)),
        ],
        compiler_params=pltpu.CompilerParams(
            collective_id=0, has_side_effects=True, vmem_limit_bytes=62 * 1024 * 1024
        ),
        name="weight_grad",
    )(features, cotangent)


def solution(mesh):
    return jax.shard_map(
        local,
        mesh=mesh,
        in_specs=(P(("row", "col"), None), P(("row", "col"), None)),
        out_specs=P("row", "col"),
        check_vma=False,
    )
```
